32 devices in a mesh: ba: 8 (over z, core), ha: 4 (over y, x).
Axes of the slice: x: 2, y: 2, z: 4, core: 2. Of those that a mesh axis runs over, the one named last changes fastest.
Arguments:
- queries: bfloat16 [2048, 64, 576], P('ba', 'ha'), may hold values from -6 to 6
- out_grad: bfloat16 [2048, 64, 512], P('ba', 'ha'), may hold values from -1.1953125 to 1.1953125
- out_saved: bfloat16 [2048, 64, 512], P('ba', 'ha'), may hold values from -3 to 3
- logsumexp: float32 [2048, 64], P('ba', 'ha'), may hold values from 7 to 9
- parents: int32 [2048], P('ba'), may hold values from 0 to 511, as said below
- latents: bfloat16 [512, 576], P(('ba', 'ha')), may hold values from -6 to 6
- hidden: bfloat16 [512, 7168], P('ba', 'ha'), may hold values from -6 to 6
- latent_weight: bfloat16 [576, 7168], P(None, 'ha'), may hold values from -0.0625 to 0.0625
Outputs:
- query_grad: bfloat16 [2048, 64, 576], P('ba', 'ha')
- weight_grad: bfloat16 [576, 7168], P('ba', 'ha')
- input_grad: bfloat16 [512, 7168], P('ba', 'ha')
The draws below stay inside these ranges and needn't reach their ends.
Inputs may be any that keep to these rules, and one draw needn't show every extreme that they name: `parents`: the 32 tokens of each aligned block of 32 share one value; some token has 0 and some has 511.
All inputs are finite; a program needn't handle non-finite values.
Results may differ from the reference program's by a relative error of at most 0.0067.
Values may be sent and summed in bfloat16 or wider, within the bound.
No kernel may reach another device: no remote copies, remote signals or barrier semaphores. Data moves between devices by JAX's collectives and lax.ppermute only.
A program may use at most 64 MiB of HBM per device.

```python
import jax
import jax.numpy as jnp
from jax import lax

RANK = 512
ROPE = 64
HEADS = 64
HID = 7168
BRANCH_LEN = 32
TOK_DEV = 256
LAT = 576
TOKENS = 2048
PREFIX = 512


def draw_parents(key, part):
    first_key, second_key = jax.random.split(jax.random.fold_in(key, 17), 2)
    branch_total = TOKENS // BRANCH_LEN
    device_total = TOKENS // TOK_DEV
    depths = jax.random.randint(first_key, (device_total,), 1, 5)
    picks = jax.random.randint(second_key, (branch_total, 4), 0, PREFIX)
    owner = jnp.arange(branch_total, dtype=jnp.int32) * BRANCH_LEN // TOK_DEV
    chosen = jnp.arange(4, dtype=jnp.int32)[None, :] < depths[owner][:, None]
    forks = jnp.min(jnp.where(chosen, picks, PREFIX), axis=1)
    forks = forks.at[0].set(PREFIX - 1)
    forks = forks.at[branch_total - 1].set(0)
    return jnp.repeat(forks, BRANCH_LEN).astype(jnp.int32)


def steps_of(rng, extent, cuts, low, top_value):
    gain, own = 1.0, jax.random.fold_in(rng, 6)
    for axis_at, parts in cuts:
        heights = jnp.exp(jax.random.uniform(jax.random.fold_in(own, axis_at), (parts,), jnp.float32, low / len(cuts), top_value / len(cuts)))
        gain = gain * jnp.repeat(heights, extent[axis_at] // parts).reshape([-1 if axis == axis_at else 1 for axis in range(len(extent))])
    return gain


def centred(key, dims, spread, reach, cuts=(), kind=jnp.bfloat16):
    array = spread * jax.random.normal(key, dims, jnp.float32)
    if cuts:
        array = array * steps_of(key, dims, cuts, -0.22, 0.18)
    return jnp.clip(array, -reach, reach).astype(kind)


def setup_inputs(seed: int = 0) -> dict:
    seeds = jax.random.split(jax.random.key(seed), 9)
    queries = centred(seeds[0], (TOKENS, HEADS, LAT), 1.0, 6.0, ((0, 8), (1, 4)))
    out_grad = centred(seeds[1], (TOKENS, HEADS, RANK), 0.2, 1.1953125, ((0, 8), (1, 4)))
    out_saved = centred(seeds[2], (TOKENS, HEADS, RANK), 0.5, 3.0, ((0, 8), (1, 4)))
    logsumexp = jnp.clip(7.0 + 2.0 * jax.random.uniform(seeds[3], (TOKENS, HEADS), jnp.float32) ** steps_of(seeds[3], (TOKENS, HEADS), ((0, 8), (1, 4)), -0.2, 0.2), 7.0, 9.0)
    parents = draw_parents(jax.random.fold_in(seeds[8], 71), 0)
    latents = centred(seeds[5], (PREFIX, LAT), 1.0, 6.0, ((0, 32),))
    hidden = centred(seeds[6], (PREFIX, HID), 1.0, 6.0, ((0, 8), (1, 4)))
    latent_weight = centred(seeds[7], (LAT, HID), HID ** -0.5, 0.0625, ((1, 4),))
    return dict(queries=queries, out_grad=out_grad, out_saved=out_saved, logsumexp=logsumexp, parents=parents, latents=latents, hidden=hidden, latent_weight=latent_weight)


softmax_scale = 192.0 ** -0.5


def reference(queries, out_grad, out_saved, logsumexp, parents, latents, hidden, latent_weight):
    key_index = jnp.arange(latents.shape[0], dtype=jnp.int32)
    visible = key_index[None, :] <= parents[:, None]

    def per_head(summed, head_args):
        query_head, grad_head, saved_head, lse_head = head_args
        scores = jnp.dot(query_head, latents.T, preferred_element_type=jnp.float32) * softmax_scale
        weights = jnp.where(visible, jnp.exp(scores - lse_head[:, None]), jnp.float32(0.0))
        grad_prob = jnp.dot(grad_head, latents[:, :RANK].T, preferred_element_type=jnp.float32)
        deltas = jnp.sum(saved_head.astype(jnp.float32) * grad_head.astype(jnp.float32), axis=1)
        grad_score = (weights * (grad_prob - deltas[:, None])).astype(jnp.bfloat16)
        query_head_grad = (softmax_scale * jnp.dot(grad_score, latents, preferred_element_type=jnp.float32)).astype(jnp.bfloat16)
        value_part = jnp.dot(weights.astype(jnp.bfloat16).T, grad_head, preferred_element_type=jnp.float32)
        key_grad = softmax_scale * jnp.dot(grad_score.T, query_head, preferred_element_type=jnp.float32)
        key_grad = key_grad + jnp.pad(value_part, ((0, 0), (0, ROPE)))
        return summed + key_grad, query_head_grad

    head_inputs = (jnp.transpose(queries, (1, 0, 2)), jnp.transpose(out_grad, (1, 0, 2)),
                   jnp.transpose(out_saved, (1, 0, 2)), jnp.transpose(logsumexp, (1, 0)))
    initial = jnp.zeros((latents.shape[0], latents.shape[1]), jnp.float32)
    latent_sum, stacked = lax.scan(per_head, initial, head_inputs)
    query_grad = jnp.transpose(stacked, (1, 0, 2))
    latent_grad = latent_sum.astype(jnp.bfloat16)
    weight_grad = jnp.dot(latent_grad.T, hidden, preferred_element_type=jnp.float32).astype(jnp.bfloat16)
    input_grad = jnp.dot(latent_grad, latent_weight, preferred_element_type=jnp.float32).astype(jnp.bfloat16)
    return (query_grad, weight_grad, input_grad)
```

```python
import jax
import jax.numpy as jnp
from jax import lax
from jax.experimental import pallas as pl
from jax.experimental.pallas import tpu as pltpu
from jax.sharding import PartitionSpec as P

BRANCH = 32
LANES = 128
GROUP = LANES // BRANCH
KEY_TILE = 256


softmax_scale = 192.0 ** (-0.5)

F32 = jnp.float32
BF16 = jnp.bfloat16


HBM = pl.BlockSpec(memory_space=pltpu.HBM)
VMEM = pl.BlockSpec(memory_space=pltpu.VMEM)
SMEM = pl.BlockSpec(memory_space=pltpu.SMEM)


def params(mib):
    return pltpu.CompilerParams(vmem_limit_bytes=mib * 1024 * 1024)


def cost(flops, nbytes):
    return pl.CostEstimate(flops=int(flops), bytes_accessed=int(nbytes), transcendentals=0)


def swap_matrix(shape=(GROUP * LANES, GROUP * LANES)):
    row = lax.broadcasted_iota(jnp.int32, shape, 0)
    col = lax.broadcasted_iota(jnp.int32, shape, 1)
    swapped = (
        jnp.bitwise_and(jnp.right_shift(col, 5), 3) * LANES
        + jnp.right_shift(col, 7) * BRANCH
        + jnp.bitwise_and(col, BRANCH - 1)
    )
    return jnp.where(row == swapped, F32(1), F32(0)).astype(BF16)


def pack_queries(queries_t):
    heads, width, tokens = queries_t.shape
    halves, groups, chunks = tokens // LANES, heads // GROUP, 6
    rows = width // chunks

    def body(q_hbm, out_ref, q_ref, sems, perm):
        def copy(d):
            at = pl.ds(pl.multiple_of(d * rows, 16), rows)
            return pltpu.make_async_copy(q_hbm.at[:, at, :], q_ref.at[:, at, :], sems.at[d])

        for d in range(chunks):
            copy(d).start()
        perm[...] = swap_matrix()

        @pl.loop(0, chunks)
        def _(d):
            copy(d).wait()
            at = pl.ds(pl.multiple_of(d * rows, 16), rows)
            wide = jnp.concatenate(
                [
                    jnp.concatenate(
                        [q_ref[g * GROUP + h, at, a * LANES : (a + 1) * LANES] for h in range(GROUP)],
                        axis=1,
                    )
                    for a in range(halves)
                    for g in range(groups)
                ],
                axis=0,
            )
            mixed = jnp.dot(wide, perm[...], preferred_element_type=F32).astype(BF16)
            for a in range(halves):
                for g in range(groups):
                    top = (a * groups + g) * rows
                    for b in range(GROUP):
                        out_ref[a * GROUP + b, at, g * LANES : (g + 1) * LANES] = mixed[
                            top : top + rows, b * LANES : (b + 1) * LANES
                        ]

    return pl.pallas_call(
        body,
        in_specs=[HBM],
        out_specs=VMEM,
        out_shape=jax.ShapeDtypeStruct((tokens // BRANCH, width, heads * BRANCH), BF16),
        scratch_shapes=[
            pltpu.VMEM((heads, width, tokens), BF16),
            pltpu.SemaphoreType.DMA((chunks,)),
            pltpu.VMEM((GROUP * LANES, GROUP * LANES), BF16),
        ],
        compiler_params=params(16),
        cost_estimate=cost(2 * heads * tokens * width * 512, 4 * heads * tokens * width),
        name="pack_queries",
    )(pltpu.with_memory_space_constraint(queries_t, pltpu.HBM))


def pack_grads(grad_rows, saved_rows, heads):
    rows, rank = grad_rows.shape
    cols = heads * BRANCH
    branches = rows // cols
    head_bits = heads.bit_length() - 1

    def body(g_hbm, o_hbm, out_ref, delta_ref, g_ref, o_ref, sems, perm):
        def copies(b):
            at = pl.ds(pl.multiple_of(b * cols, 16), cols)
            return (
                pltpu.make_async_copy(g_hbm.at[at, :], g_ref.at[at, :], sems.at[0, b]),
                pltpu.make_async_copy(o_hbm.at[at, :], o_ref.at[at, :], sems.at[1, b]),
            )

        for b in range(branches):
            for copy in copies(b):
                copy.start()
        row = lax.broadcasted_iota(jnp.int32, (cols, cols), 0)
        col = lax.broadcasted_iota(jnp.int32, (cols, cols), 1)
        source = jnp.left_shift(jnp.bitwise_and(col, BRANCH - 1), head_bits) + jnp.right_shift(col, 5)
        perm[...] = jnp.where(row == source, F32(1), F32(0)).astype(BF16)

        @pl.loop(0, branches)
        def _(b):
            for copy in copies(b):
                copy.wait()
            at = pl.ds(pl.multiple_of(b * cols, 16), cols)
            grads = g_ref[at, :]
            out_ref[b] = lax.dot_general(
                grads, perm[...], (((0,), (0,)), ((), ())), preferred_element_type=F32
            ).astype(BF16)
            delta = jnp.sum(o_ref[at, :].astype(F32) * grads.astype(F32), axis=1, keepdims=True)
            high = delta.astype(BF16)
            rest = delta - high.astype(F32)
            mid = rest.astype(BF16)
            low = (rest - mid.astype(F32)).astype(BF16)
            lane = lax.broadcasted_iota(jnp.int32, (cols, LANES), 1)
            parts = jnp.where(
                lane == 0,
                high.astype(F32),
                jnp.where(lane == 1, mid.astype(F32), jnp.where(lane == 2, low.astype(F32), F32(0))),
            ).astype(BF16)
            moved = lax.dot_general(
                parts, perm[...], (((0,), (0,)), ((), ())), preferred_element_type=F32
            )
            delta_ref[b] = moved[0:1] + moved[1:2] + moved[2:3]

    return pl.pallas_call(
        body,
        in_specs=[HBM, HBM],
        out_specs=[VMEM, VMEM],
        out_shape=[
            jax.ShapeDtypeStruct((branches, rank, cols), BF16),
            jax.ShapeDtypeStruct((branches, 1, cols), F32),
        ],
        scratch_shapes=[
            pltpu.VMEM((rows, rank), BF16),
            pltpu.VMEM((rows, rank), BF16),
            pltpu.SemaphoreType.DMA((2, branches)),
            pltpu.VMEM((cols, cols), BF16),
        ],
        compiler_params=params(20),
        cost_estimate=cost(2 * rows * rank * cols, 6 * rows * rank),
        name="pack_grads",
    )(
        pltpu.with_memory_space_constraint(grad_rows, pltpu.HBM),
        pltpu.with_memory_space_constraint(saved_rows, pltpu.HBM),
    )


def attend(place, parents, own_keys, other_keys, packed_q, packed_g, lse, deltas, sizes):
    ba, ha = sizes
    columns = ba // 2
    branches, width, cols = packed_q.shape
    rank = packed_g.shape[1]
    slots, piece, _ = own_keys.shape
    prefix = 2 * slots * piece
    key_tile = min(KEY_TILE, prefix)
    tiles = prefix // key_tile
    keys_ba = prefix // ba
    width_ba = width // ba
    half = width * keys_ba // LANES
    payload = 2 * half
    part = payload // ha

    def body(place_ref, parents_ref, own_ref, other_ref, q_ref, g_ref, lse_ref, delta_ref,
             send_ref, score_ref, keys, acc_q, acc_g, pack):
        me_ba, me_ha = place_ref[0], place_ref[1]
        me_col, me_core = jnp.right_shift(me_ba, 1), jnp.bitwise_and(me_ba, 1)

        for core_at, ref in enumerate((own_ref, other_ref)):
            for hr in range(ha):
                for zr in range(columns):
                    ba_at = 2 * jnp.bitwise_xor(me_col, zr) + jnp.bitwise_xor(me_core, core_at)
                    at = ba_at * ha + jnp.bitwise_xor(me_ha, hr)
                    keys[pl.ds(pl.multiple_of(at * piece, piece), piece), :] = ref[hr * columns + zr]
        acc_q[...] = jnp.zeros_like(acc_q)
        acc_g[...] = jnp.zeros_like(acc_g)

        @pl.loop(0, branches)
        def _(b):
            limit = parents_ref[b * BRANCH]
            for kt in range(tiles):
                rows = slice(kt * key_tile, (kt + 1) * key_tile)

                @pl.when(limit >= kt * key_tile)
                def _(rows=rows, kt=kt):
                    key_block = keys[rows, :]
                    scores = jnp.dot(key_block, q_ref[b], preferred_element_type=F32) * softmax_scale
                    at = kt * key_tile + lax.broadcasted_iota(jnp.int32, scores.shape, 0)
                    prob = jnp.where(at <= limit, jnp.exp(scores - lse_ref[b]), F32(0))
                    grad_prob = jnp.dot(key_block[:, :rank], g_ref[b], preferred_element_type=F32)
                    grad_score = (prob * (grad_prob - delta_ref[b])).astype(BF16)
                    score_ref[b, rows, :] = grad_score
                    across = (((1,), (1,)), ((), ()))
                    acc_q[:, rows] += lax.dot_general(
                        q_ref[b], grad_score, across, preferred_element_type=F32
                    )
                    acc_g[:, rows] += lax.dot_general(
                        g_ref[b], prob.astype(BF16), across, preferred_element_type=F32
                    )

                @pl.when(limit < kt * key_tile)
                def _(rows=rows):
                    score_ref[b, rows, :] = jnp.zeros((key_tile, cols), BF16)

        acc_q[...] = acc_q[...] * softmax_scale
        acc_q[:rank, :] += acc_g[...]
        lane = lax.broadcasted_iota(jnp.int32, (half, LANES), 1)
        per_tile = LANES // keys_ba
        for at in range(ba):
            tile = acc_q[:, (at // per_tile) * LANES : (at // per_tile + 1) * LANES]
            first = at % per_tile
            block = jnp.zeros((half, LANES), F32)
            for s in range(per_tile):
                strip = tile[s * half : (s + 1) * half, :]
                shift = ((s - first) * keys_ba) % LANES
                if shift:
                    strip = pltpu.roll(strip, shift, axis=1)
                block = jnp.where((lane >= s * keys_ba) & (lane < (s + 1) * keys_ba), strip, block)
            pack[:half, :] = block
            for l in range(prefix // LANES):
                pack[half + l * width_ba : half + (l + 1) * width_ba, :] = acc_q[
                    at * width_ba : (at + 1) * width_ba, l * LANES : (l + 1) * LANES
                ]
            to_core = jnp.bitwise_xor(me_core, at % 2)
            to_col = jnp.bitwise_xor(me_col, at // 2)
            for h in range(ha):
                send_ref[to_core, jnp.bitwise_xor(me_ha, h), to_col] = pack[
                    h * part : (h + 1) * part, :
                ]

    return pl.pallas_call(
        body,
        in_specs=[SMEM, SMEM] + [VMEM] * 6,
        out_specs=[VMEM, VMEM, VMEM],
        out_shape=[
            jax.ShapeDtypeStruct((2, ha, columns, part, LANES), F32),
            jax.ShapeDtypeStruct((branches, prefix, cols), BF16),
            jax.ShapeDtypeStruct((prefix, width), BF16),
        ],
        scratch_shapes=[
            pltpu.VMEM((width, prefix), F32),
            pltpu.VMEM((rank, prefix), F32),
            pltpu.VMEM((payload, LANES), F32),
        ],
        compiler_params=params(24),
        cost_estimate=cost(8 * branches * cols * prefix * width, 3 * branches * cols * width * 2),
        name="attend",
    )(place, parents, own_keys, other_keys, packed_q, packed_g, lse, deltas)


def exchange(tiles):
    lane = lax.broadcasted_iota(jnp.int32, tiles[0].shape, 1)
    bit, tiles = GROUP // 2, list(tiles)
    while bit:
        width = bit * BRANCH
        low = jnp.bitwise_and(lane, width) == 0
        out = list(tiles)
        for at in range(GROUP):
            if not at & bit:
                a, b = tiles[at], tiles[at | bit]
                out[at] = jnp.where(low, a, pltpu.roll(b, width, axis=1))
                out[at | bit] = jnp.where(low, pltpu.roll(a, LANES - width, axis=1), b)
        tiles, bit = out, bit // 2
    return tiles


def query_gradient(before, steps, keys, grad_score, heads):
    branches, prefix, _ = grad_score.shape
    width = keys.shape[1]
    tokens = branches * BRANCH
    halves = tokens // LANES
    first, last = steps

    def body(k_ref, s_ref, *refs):
        out_hbm, keys_t, slots, sems = refs[-4:]
        keys_t[...] = jnp.transpose(k_ref[...], (1, 0))

        def copy(g):
            at = (g - first) % 2
            return pltpu.make_async_copy(
                slots.at[at], out_hbm.at[pl.ds(g * GROUP, GROUP)], sems.at[at]
            )

        for g in range(first, last):
            if g - first >= 2:
                copy(g - 2).wait()
            for a in range(halves):
                wide = jnp.concatenate(
                    [s_ref[a * GROUP + b, :, g * LANES : (g + 1) * LANES] for b in range(GROUP)], axis=1
                )
                grads = softmax_scale * jnp.dot(keys_t[...], wide, preferred_element_type=F32)
                tiles = exchange([grads[:, b * LANES : (b + 1) * LANES] for b in range(GROUP)])
                for h in range(GROUP):
                    slots[(g - first) % 2, h, :, a * LANES : (a + 1) * LANES] = tiles[h].astype(BF16)
            copy(g).start()
        for g in range(max(first, last - 2), last):
            copy(g).wait()

    return pl.pallas_call(
        body,
        in_specs=[VMEM, VMEM] + ([] if before is None else [HBM]),
        out_specs=HBM,
        out_shape=jax.ShapeDtypeStruct((heads, width, tokens), BF16),
        input_output_aliases={} if before is None else {2: 0},
        scratch_shapes=[
            pltpu.VMEM((width, prefix), BF16),
            pltpu.VMEM((2, GROUP, width, tokens), BF16),
            pltpu.SemaphoreType.DMA((2,)),
        ],
        compiler_params=params(16),
        cost_estimate=cost(
            2 * (last - first) * GROUP * tokens * prefix * width, (last - first) * GROUP * tokens * width * 2
        ),
        name="query_gradient",
    )(keys, grad_score, *([] if before is None else [before]))


def project(place, parts, hidden_sets, order, latent_weight, sizes, prefix):
    ba, ha = sizes
    width, columns = latent_weight.shape
    keys_ba, width_ba = prefix // ba, width // ba
    part = parts[0].shape[0]
    half = part * ha // 2

    def body(place_ref, *refs):
        part_refs = refs[:ha]
        own_ref, other_ref, weight_ref, wgrad_ref, igrad_ref, pack, hid = refs[ha:]
        me_ba, me_ha = place_ref[0], place_ref[1]
        for hr in range(ha):
            at = jnp.bitwise_xor(me_ha, hr) * part
            pack[pl.ds(pl.multiple_of(at, 8), part), :] = part_refs[hr][...].astype(F32)
        for core_at, ref in enumerate((own_ref, other_ref)):
            for slot, zr in enumerate(order):
                at = jnp.bitwise_xor(me_ba, 2 * zr + core_at) * keys_ba
                hid[pl.ds(pl.multiple_of(at, 8), keys_ba), :] = ref[slot]
        grad_columns = jnp.concatenate(
            [
                pack[half + l * width_ba : half + (l + 1) * width_ba, :]
                for l in range(prefix // LANES)
            ],
            axis=1,
        ).astype(BF16)
        wgrad_ref[...] = jnp.dot(grad_columns, hid[...], preferred_element_type=F32).astype(BF16)
        rows_t = jnp.concatenate(
            [
                pack[:half, s * keys_ba : (s + 1) * keys_ba]
                for s in range(LANES // keys_ba)
            ],
            axis=0,
        ).astype(BF16)
        igrad_ref[...] = lax.dot_general(
            rows_t, weight_ref[...], (((0,), (0,)), ((), ())), preferred_element_type=F32
        ).astype(BF16)

    return pl.pallas_call(
        body,
        in_specs=[SMEM] + [VMEM] * (ha + 3),
        out_specs=[VMEM, VMEM],
        out_shape=[
            jax.ShapeDtypeStruct((width_ba, columns), BF16),
            jax.ShapeDtypeStruct((keys_ba, columns), BF16),
        ],
        scratch_shapes=[
            pltpu.VMEM((part * ha, LANES), F32),
            pltpu.VMEM((prefix, columns), BF16),
        ],
        compiler_params=params(24),
        cost_estimate=cost(4 * width * keys_ba * columns, 4 * width * columns),
        name="project",
    )(place, *parts, *hidden_sets, latent_weight)


def on_device(sizes, queries, out_grad, out_saved, logsumexp, parents, latents, hidden, latent_weight):
    ba, ha = sizes
    columns = ba // 2
    tokens, heads, _ = queries.shape
    rank = out_grad.shape[2]
    branches, cols = tokens // BRANCH, heads * BRANCH
    prefix = latents.shape[0] * ba * ha

    def over_core(x):
        return lax.ppermute(x, "ba", [(i, i ^ 1) for i in range(ba)])

    def over_column(x, k):
        return lax.ppermute(x, "ba", [(i, i ^ (2 * k)) for i in range(ba)])

    def over_ha(x, k):
        return lax.ppermute(x, "ha", [(i, i ^ k) for i in range(ha)])

    def total(terms):
        return sum(t.astype(F32) for t in terms).astype(BF16)

    place = jnp.stack([lax.axis_index("ba"), lax.axis_index("ha")]).astype(jnp.int32)

    keys = jnp.stack([latents] + [over_column(latents, k) for k in range(1, columns)])
    keys = jnp.concatenate([keys] + [over_ha(keys, k) for k in range(1, ha)])
    other_keys = over_core(keys)

    packed_q = pack_queries(jnp.transpose(queries, (1, 2, 0)))
    packed_g, deltas = pack_grads(
        out_grad.reshape(tokens * heads, rank), out_saved.reshape(tokens * heads, rank), heads
    )
    lse = jnp.transpose(logsumexp.T.reshape(heads, branches, BRANCH), (1, 0, 2)).reshape(branches, 1, cols)

    hidden_all, order = hidden[None], [0]
    step = columns // 2
    while step:
        hidden_all = jnp.concatenate([hidden_all, over_column(hidden_all, step)])
        order = order + [k ^ step for k in order]
        step //= 2
    other_hidden = over_core(hidden_all)

    send, grad_score, keys = attend(
        place, parents, keys, other_keys, packed_q, packed_g, lse, deltas, sizes
    )
    query_grad, groups = None, heads // GROUP
    for steps in ((0, 1), (1, groups)):
        query_grad = query_gradient(query_grad, steps, keys, grad_score, heads)

    chip = (send[0] + over_core(send[1])).astype(BF16)
    plane = total([chip[0]] + [over_ha(chip[k], k) for k in range(1, ha)])
    owned = total([plane[0]] + [over_column(plane[k], k) for k in range(1, columns)])
    parts = [owned] + [over_ha(owned, k) for k in range(1, ha)]
    weight_grad, input_grad = project(
        place, parts, (hidden_all, other_hidden), order, latent_weight, sizes, prefix
    )
    return (jnp.transpose(query_grad, (2, 0, 1)), weight_grad, input_grad)


def solution(mesh):
    sizes = (mesh.shape["ba"], mesh.shape["ha"])

    def step(*args):
        return on_device(sizes, *args)

    step = jax.shard_map(
        step,
        mesh=mesh,
        in_specs=(
            P("ba", "ha", None),
            P("ba", "ha", None),
            P("ba", "ha", None),
            P("ba", "ha"),
            P("ba"),
            P(("ba", "ha"), None),
            P("ba", "ha"),
            P(None, "ha"),
        ),
        out_specs=(P("ba", "ha", None), P("ba", "ha"), P("ba", "ha")),
        check_vma=False,
    )
    return step
```

```python
import jax
import jax.numpy as jnp
from jax import lax
from jax.experimental import pallas as pl
from jax.experimental.pallas import tpu as pltpu
from jax.sharding import PartitionSpec as P

BRANCH = 32
LANES = 128
GROUP = LANES // BRANCH
KEY_TILE = 256


softmax_scale = 192.0 ** (-0.5)

F32 = jnp.float32
BF16 = jnp.bfloat16


HBM = pl.BlockSpec(memory_space=pltpu.HBM)
VMEM = pl.BlockSpec(memory_space=pltpu.VMEM)
SMEM = pl.BlockSpec(memory_space=pltpu.SMEM)


def params(mib):
    return pltpu.CompilerParams(vmem_limit_bytes=mib * 1024 * 1024)


def cost(flops, nbytes):
    return pl.CostEstimate(flops=int(flops), bytes_accessed=int(nbytes), transcendentals=0)


def swap_matrix(shape=(GROUP * LANES, GROUP * LANES)):
    row = lax.broadcasted_iota(jnp.int32, shape, 0)
    col = lax.broadcasted_iota(jnp.int32, shape, 1)
    swapped = (
        jnp.bitwise_and(jnp.right_shift(col, 5), 3) * LANES
        + jnp.right_shift(col, 7) * BRANCH
        + jnp.bitwise_and(col, BRANCH - 1)
    )
    return jnp.where(row == swapped, F32(1), F32(0)).astype(BF16)


def exchange(tiles):
    lane = lax.broadcasted_iota(jnp.int32, tiles[0].shape, 1)
    bit, tiles = GROUP // 2, list(tiles)
    while bit:
        width = bit * BRANCH
        low = jnp.bitwise_and(lane, width) == 0
        out = list(tiles)
        for at in range(GROUP):
            if not at & bit:
                a, b = tiles[at], tiles[at | bit]
                out[at] = jnp.where(low, a, pltpu.roll(b, width, axis=1))
                out[at | bit] = jnp.where(low, pltpu.roll(a, LANES - width, axis=1), b)
        tiles, bit = out, bit // 2
    return tiles


def pack_queries(queries_t):
    heads, width, tokens = queries_t.shape
    halves, groups, chunks = tokens // LANES, heads // GROUP, 6
    rows = width // chunks

    def body(q_hbm, out_ref, q_ref, sems, perm):
        def copy(d):
            at = pl.ds(pl.multiple_of(d * rows, 16), rows)
            return pltpu.make_async_copy(q_hbm.at[:, at, :], q_ref.at[:, at, :], sems.at[d])

        for d in range(chunks):
            copy(d).start()
        perm[...] = swap_matrix()

        @pl.loop(0, chunks)
        def _(d):
            copy(d).wait()
            at = pl.ds(pl.multiple_of(d * rows, 16), rows)
            wide = jnp.concatenate(
                [
                    jnp.concatenate(
                        [q_ref[g * GROUP + h, at, a * LANES : (a + 1) * LANES] for h in range(GROUP)],
                        axis=1,
                    )
                    for a in range(halves)
                    for g in range(groups)
                ],
                axis=0,
            )
            mixed = jnp.dot(wide, perm[...], preferred_element_type=F32).astype(BF16)
            for a in range(halves):
                for g in range(groups):
                    top = (a * groups + g) * rows
                    for b in range(GROUP):
                        out_ref[a * GROUP + b, at, g * LANES : (g + 1) * LANES] = mixed[
                            top : top + rows, b * LANES : (b + 1) * LANES
                        ]

    return pl.pallas_call(
        body,
        in_specs=[HBM],
        out_specs=VMEM,
        out_shape=jax.ShapeDtypeStruct((tokens // BRANCH, width, heads * BRANCH), BF16),
        scratch_shapes=[
            pltpu.VMEM((heads, width, tokens), BF16),
            pltpu.SemaphoreType.DMA((chunks,)),
            pltpu.VMEM((GROUP * LANES, GROUP * LANES), BF16),
        ],
        compiler_params=params(16),
        cost_estimate=cost(2 * heads * tokens * width * 512, 4 * heads * tokens * width),
        name="pack_queries",
    )(pltpu.with_memory_space_constraint(queries_t, pltpu.HBM))


def pack_grads(grad_rows, saved_rows, lse_t):
    heads, tokens = lse_t.shape
    groups = heads // GROUP
    rows, rank = grad_rows.shape
    cols = heads * BRANCH
    branches = rows // cols
    head_bits = heads.bit_length() - 1

    def body(g_hbm, o_hbm, l_hbm, out_ref, delta_ref, lse_ref, g_ref, o_ref, l_ref, sems, l_sem, perm):
        lse_copy = pltpu.make_async_copy(l_hbm, l_ref, l_sem)
        lse_copy.start()

        def copies(b):
            at = pl.ds(pl.multiple_of(b * cols, 16), cols)
            return (
                pltpu.make_async_copy(g_hbm.at[at, :], g_ref.at[at, :], sems.at[0, b]),
                pltpu.make_async_copy(o_hbm.at[at, :], o_ref.at[at, :], sems.at[1, b]),
            )

        for b in range(branches):
            for copy in copies(b):
                copy.start()
        row = lax.broadcasted_iota(jnp.int32, (cols, cols), 0)
        col = lax.broadcasted_iota(jnp.int32, (cols, cols), 1)
        source = jnp.left_shift(jnp.bitwise_and(col, BRANCH - 1), head_bits) + jnp.right_shift(col, 5)
        perm[...] = jnp.where(row == source, F32(1), F32(0)).astype(BF16)

        @pl.loop(0, branches)
        def _(b):
            for copy in copies(b):
                copy.wait()
            at = pl.ds(pl.multiple_of(b * cols, 16), cols)
            grads = g_ref[at, :]
            out_ref[b] = lax.dot_general(
                grads, perm[...], (((0,), (0,)), ((), ())), preferred_element_type=F32
            ).astype(BF16)
            delta = jnp.sum(o_ref[at, :].astype(F32) * grads.astype(F32), axis=1, keepdims=True)
            high = delta.astype(BF16)
            rest = delta - high.astype(F32)
            mid = rest.astype(BF16)
            low = (rest - mid.astype(F32)).astype(BF16)
            lane = lax.broadcasted_iota(jnp.int32, (cols, LANES), 1)
            parts = jnp.where(
                lane == 0,
                high.astype(F32),
                jnp.where(lane == 1, mid.astype(F32), jnp.where(lane == 2, low.astype(F32), F32(0))),
            ).astype(BF16)
            moved = lax.dot_general(
                parts, perm[...], (((0,), (0,)), ((), ())), preferred_element_type=F32
            )
            delta_ref[b] = moved[0:1] + moved[1:2] + moved[2:3]

        lse_copy.wait()
        for a in range(tokens // LANES):
            tile = l_ref[:, a * LANES : (a + 1) * LANES]
            picked = exchange(
                [
                    jnp.concatenate(
                        [tile[g * GROUP + h : g * GROUP + h + 1] for g in range(groups)], axis=0
                    )
                    for h in range(GROUP)
                ]
            )
            for b in range(GROUP):
                lse_ref[a * GROUP + b] = picked[b]

    return pl.pallas_call(
        body,
        in_specs=[HBM, HBM, HBM],
        out_specs=[VMEM, VMEM, VMEM],
        out_shape=[
            jax.ShapeDtypeStruct((branches, rank, cols), BF16),
            jax.ShapeDtypeStruct((branches, 1, cols), F32),
            jax.ShapeDtypeStruct((branches, groups, LANES), F32),
        ],
        scratch_shapes=[
            pltpu.VMEM((rows, rank), BF16),
            pltpu.VMEM((rows, rank), BF16),
            pltpu.VMEM((heads, tokens), F32),
            pltpu.SemaphoreType.DMA((2, branches)),
            pltpu.SemaphoreType.DMA,
            pltpu.VMEM((cols, cols), BF16),
        ],
        compiler_params=params(20),
        cost_estimate=cost(2 * rows * rank * cols, 6 * rows * rank),
        name="pack_grads",
    )(
        pltpu.with_memory_space_constraint(grad_rows, pltpu.HBM),
        pltpu.with_memory_space_constraint(saved_rows, pltpu.HBM),
        pltpu.with_memory_space_constraint(lse_t, pltpu.HBM),
    )


def attend(place, parents, own_keys, other_keys, packed_q, packed_g, lse, deltas, sizes):
    ba, ha = sizes
    columns = ba // 2
    branches, width, cols = packed_q.shape
    rank = packed_g.shape[1]
    slots, piece, _ = own_keys.shape
    prefix = 2 * slots * piece
    key_tile = min(KEY_TILE, prefix)
    tiles = prefix // key_tile
    keys_ba = prefix // ba
    width_ba = width // ba
    half = width * keys_ba // LANES
    payload = 2 * half
    part = payload // ha

    def body(place_ref, parents_ref, own_ref, other_ref, q_ref, g_ref, lse_ref, delta_ref,
             send_ref, score_ref, keys, acc_q, acc_g, pack):
        me_ba, me_ha = place_ref[0], place_ref[1]
        me_col, me_core = jnp.right_shift(me_ba, 1), jnp.bitwise_and(me_ba, 1)

        for core_at, ref in enumerate((own_ref, other_ref)):
            for hr in range(ha):
                for zr in range(columns):
                    ba_at = 2 * jnp.bitwise_xor(me_col, zr) + jnp.bitwise_xor(me_core, core_at)
                    at = ba_at * ha + jnp.bitwise_xor(me_ha, hr)
                    keys[pl.ds(pl.multiple_of(at * piece, piece), piece), :] = ref[hr * columns + zr]
        acc_q[...] = jnp.zeros_like(acc_q)
        acc_g[...] = jnp.zeros_like(acc_g)

        @pl.loop(0, branches)
        def _(b):
            limit = parents_ref[b * BRANCH]
            lse_row = jnp.concatenate([lse_ref[b, g : g + 1] for g in range(cols // LANES)], axis=1)
            for kt in range(tiles):
                start = kt * key_tile
                for size in (key_tile // 2, key_tile):
                    low = start if size < key_tile else start + key_tile // 2
                    wanted = limit >= low
                    if size < key_tile:
                        wanted &= limit < start + key_tile // 2

                    @pl.when(wanted)
                    def _(rows=slice(start, start + size), size=size, start=start):
                        key_block = keys[rows, :]
                        scores = jnp.dot(key_block, q_ref[b], preferred_element_type=F32) * softmax_scale
                        at = start + lax.broadcasted_iota(jnp.int32, scores.shape, 0)
                        prob = jnp.where(at <= limit, jnp.exp(scores - lse_row), F32(0))
                        grad_prob = jnp.dot(key_block[:, :rank], g_ref[b], preferred_element_type=F32)
                        grad_score = (prob * (grad_prob - delta_ref[b])).astype(BF16)
                        score_ref[b, rows, :] = grad_score
                        if size < key_tile:
                            score_ref[b, start + size : start + key_tile, :] = jnp.zeros(
                                (key_tile - size, cols), BF16
                            )
                        across = (((1,), (1,)), ((), ()))
                        acc_q[:, rows] += lax.dot_general(
                            q_ref[b], grad_score, across, preferred_element_type=F32
                        )
                        acc_g[:, rows] += lax.dot_general(
                            g_ref[b], prob.astype(BF16), across, preferred_element_type=F32
                        )

                @pl.when(limit < start)
                def _(start=start):
                    score_ref[b, start : start + key_tile, :] = jnp.zeros((key_tile, cols), BF16)

        acc_q[...] = acc_q[...] * softmax_scale
        acc_q[:rank, :] += acc_g[...]
        lane = lax.broadcasted_iota(jnp.int32, (half, LANES), 1)
        per_tile = LANES // keys_ba
        for at in range(ba):
            tile = acc_q[:, (at // per_tile) * LANES : (at // per_tile + 1) * LANES]
            first = at % per_tile
            block = jnp.zeros((half, LANES), F32)
            for s in range(per_tile):
                strip = tile[s * half : (s + 1) * half, :]
                shift = ((s - first) * keys_ba) % LANES
                if shift:
                    strip = pltpu.roll(strip, shift, axis=1)
                block = jnp.where((lane >= s * keys_ba) & (lane < (s + 1) * keys_ba), strip, block)
            pack[:half, :] = block
            for l in range(prefix // LANES):
                pack[half + l * width_ba : half + (l + 1) * width_ba, :] = acc_q[
                    at * width_ba : (at + 1) * width_ba, l * LANES : (l + 1) * LANES
                ]
            to_core = jnp.bitwise_xor(me_core, at % 2)
            to_col = jnp.bitwise_xor(me_col, at // 2)
            for h in range(ha):
                send_ref[to_core, jnp.bitwise_xor(me_ha, h), to_col] = pack[
                    h * part : (h + 1) * part, :
                ]

    return pl.pallas_call(
        body,
        in_specs=[SMEM, SMEM] + [VMEM] * 6,
        out_specs=[VMEM, VMEM, VMEM],
        out_shape=[
            jax.ShapeDtypeStruct((2, ha, columns, part, LANES), F32),
            jax.ShapeDtypeStruct((branches, prefix, cols), BF16),
            jax.ShapeDtypeStruct((prefix, width), BF16),
        ],
        scratch_shapes=[
            pltpu.VMEM((width, prefix), F32),
            pltpu.VMEM((rank, prefix), F32),
            pltpu.VMEM((payload, LANES), F32),
        ],
        compiler_params=params(24),
        cost_estimate=cost(8 * branches * cols * prefix * width, 3 * branches * cols * width * 2),
        name="attend",
    )(place, parents, own_keys, other_keys, packed_q, packed_g, lse, deltas)


def query_gradient(before, steps, keys, grad_score, heads):
    branches, prefix, _ = grad_score.shape
    width = keys.shape[1]
    tokens = branches * BRANCH
    halves = tokens // LANES
    first, last = steps

    def body(k_ref, s_ref, *refs):
        out_hbm, keys_t, slots, sems = refs[-4:]
        keys_t[...] = jnp.transpose(k_ref[...], (1, 0))

        def copy(g):
            at = (g - first) % 2
            return pltpu.make_async_copy(
                slots.at[at], out_hbm.at[pl.ds(g * GROUP, GROUP)], sems.at[at]
            )

        for g in range(first, last):
            if g - first >= 2:
                copy(g - 2).wait()
            for a in range(halves):
                wide = jnp.concatenate(
                    [s_ref[a * GROUP + b, :, g * LANES : (g + 1) * LANES] for b in range(GROUP)], axis=1
                )
                grads = softmax_scale * jnp.dot(keys_t[...], wide, preferred_element_type=F32)
                tiles = exchange([grads[:, b * LANES : (b + 1) * LANES] for b in range(GROUP)])
                for h in range(GROUP):
                    slots[(g - first) % 2, h, :, a * LANES : (a + 1) * LANES] = tiles[h].astype(BF16)
            copy(g).start()
        for g in range(max(first, last - 2), last):
            copy(g).wait()

    return pl.pallas_call(
        body,
        in_specs=[VMEM, VMEM] + ([] if before is None else [HBM]),
        out_specs=HBM,
        out_shape=jax.ShapeDtypeStruct((heads, width, tokens), BF16),
        input_output_aliases={} if before is None else {2: 0},
        scratch_shapes=[
            pltpu.VMEM((width, prefix), BF16),
            pltpu.VMEM((2, GROUP, width, tokens), BF16),
            pltpu.SemaphoreType.DMA((2,)),
        ],
        compiler_params=params(16),
        cost_estimate=cost(
            2 * (last - first) * GROUP * tokens * prefix * width, (last - first) * GROUP * tokens * width * 2
        ),
        name="query_gradient",
    )(keys, grad_score, *([] if before is None else [before]))


def project(place, parts, hidden_sets, order, latent_weight, sizes, prefix):
    ba, ha = sizes
    width, columns = latent_weight.shape
    keys_ba, width_ba = prefix // ba, width // ba
    part = parts[0].shape[0]
    half = part * ha // 2
    middle = -(-columns // 512) * 256
    parts_of = (slice(0, middle), slice(middle, columns))

    def body(place_ref, *refs):
        part_refs = refs[:ha]
        own_ref, other_ref, weight_ref, wgrad_hbm, igrad_hbm, pack, hid, wrows, irows, sems = refs[ha:]
        me_ba, me_ha = place_ref[0], place_ref[1]
        for hr in range(ha):
            at = jnp.bitwise_xor(me_ha, hr) * part
            pack[pl.ds(pl.multiple_of(at, 8), part), :] = part_refs[hr][...].astype(F32)
        for core_at, ref in enumerate((own_ref, other_ref)):
            for slot, zr in enumerate(order):
                at = jnp.bitwise_xor(me_ba, 2 * zr + core_at) * keys_ba
                hid[pl.ds(pl.multiple_of(at, 8), keys_ba), :] = ref[slot]
        grad_columns = jnp.concatenate(
            [
                pack[half + l * width_ba : half + (l + 1) * width_ba, :]
                for l in range(prefix // LANES)
            ],
            axis=1,
        ).astype(BF16)
        rows_t = jnp.concatenate(
            [
                pack[:half, s * keys_ba : (s + 1) * keys_ba]
                for s in range(LANES // keys_ba)
            ],
            axis=0,
        ).astype(BF16)
        copies = []

        def send(buffer, out_hbm, at, value):
            buffer[:, at] = value.astype(BF16)
            copy = pltpu.make_async_copy(buffer.at[:, at], out_hbm.at[:, at], sems.at[len(copies)])
            copy.start()
            copies.append(copy)

        for at in parts_of:
            term = lax.dot_general(
                rows_t, weight_ref[:, at], (((0,), (0,)), ((), ())), preferred_element_type=F32
            )
            send(irows, igrad_hbm, at, term)
        for at in parts_of:
            send(wrows, wgrad_hbm, at, jnp.dot(grad_columns, hid[:, at], preferred_element_type=F32))
        for copy in copies:
            copy.wait()

    return pl.pallas_call(
        body,
        in_specs=[SMEM] + [VMEM] * (ha + 3),
        out_specs=[HBM, HBM],
        out_shape=[
            jax.ShapeDtypeStruct((width_ba, columns), BF16),
            jax.ShapeDtypeStruct((keys_ba, columns), BF16),
        ],
        scratch_shapes=[
            pltpu.VMEM((part * ha, LANES), F32),
            pltpu.VMEM((prefix, columns), BF16),
            pltpu.VMEM((width_ba, columns), BF16),
            pltpu.VMEM((keys_ba, columns), BF16),
            pltpu.SemaphoreType.DMA((4,)),
        ],
        compiler_params=params(24),
        cost_estimate=cost(4 * width * keys_ba * columns, 4 * width * columns),
        name="project",
    )(place, *parts, *hidden_sets, latent_weight)


def on_device(sizes, queries, out_grad, out_saved, logsumexp, parents, latents, hidden, latent_weight):
    ba, ha = sizes
    columns = ba // 2
    tokens, heads, _ = queries.shape
    rank = out_grad.shape[2]
    prefix = latents.shape[0] * ba * ha

    def over_core(x):
        return lax.ppermute(x, "ba", [(i, i ^ 1) for i in range(ba)])

    def over_column(x, k):
        return lax.ppermute(x, "ba", [(i, i ^ (2 * k)) for i in range(ba)])

    def over_ha(x, k):
        return lax.ppermute(x, "ha", [(i, i ^ k) for i in range(ha)])

    def total(terms):
        return sum(t.astype(F32) for t in terms).astype(BF16)

    place = jnp.stack([lax.axis_index("ba"), lax.axis_index("ha")]).astype(jnp.int32)

    keys = jnp.stack([latents] + [over_column(latents, k) for k in range(1, columns)])
    keys = lax.optimization_barrier(keys)
    keys = jnp.concatenate([keys] + [over_ha(keys, k) for k in range(1, ha)])
    other_keys = over_core(keys)

    packed_q = pack_queries(jnp.transpose(queries, (1, 2, 0)))
    packed_g, deltas, lse = pack_grads(
        out_grad.reshape(tokens * heads, rank), out_saved.reshape(tokens * heads, rank), logsumexp.T
    )

    hidden_all, order = hidden[None], [0]
    step = columns // 2
    while step:
        hidden_all = jnp.concatenate([hidden_all, over_column(hidden_all, step)])
        if step > 1:
            place, hidden_all = lax.optimization_barrier((place, hidden_all))
        order = order + [k ^ step for k in order]
        step //= 2
    other_hidden = over_core(hidden_all)

    send, grad_score, keys = attend(
        place, parents, keys, other_keys, packed_q, packed_g, lse, deltas, sizes
    )
    query_grad, groups = None, heads // GROUP
    for steps in ((0, 1), (1, groups)):
        query_grad = query_gradient(query_grad, steps, keys, grad_score, heads)

    chip = (send[0] + over_core(send[1])).astype(BF16)
    plane = total([chip[0]] + [over_ha(chip[k], k) for k in range(1, ha)])
    owned = total([plane[0]] + [over_column(plane[k], k) for k in range(1, columns)])
    parts = [owned] + [over_ha(owned, k) for k in range(1, ha)]
    weight_grad, input_grad = project(
        place, parts, (hidden_all, other_hidden), order, latent_weight, sizes, prefix
    )
    return (jnp.transpose(query_grad, (2, 0, 1)), weight_grad, input_grad)


def solution(mesh):
    sizes = (mesh.shape["ba"], mesh.shape["ha"])

    def step(*args):
        return on_device(sizes, *args)

    step = jax.shard_map(
        step,
        mesh=mesh,
        in_specs=(
            P("ba", "ha", None),
            P("ba", "ha", None),
            P("ba", "ha", None),
            P("ba", "ha"),
            P("ba"),
            P(("ba", "ha"), None),
            P("ba", "ha"),
            P(None, "ha"),
        ),
        out_specs=(P("ba", "ha", None), P("ba", "ha"), P("ba", "ha")),
        check_vma=False,
    )
    return step
```

```python
import jax
import jax.numpy as jnp
from jax import lax
from jax.experimental import pallas as pl
from jax.experimental.pallas import tpu as pltpu
from jax.sharding import PartitionSpec as P

BRANCH = 32
LANES = 128
GROUP = LANES // BRANCH
KEY_TILE = 256
COLUMN_CHUNK = 256


softmax_scale = 192.0 ** (-0.5)

F32 = jnp.float32
BF16 = jnp.bfloat16


HBM = pl.BlockSpec(memory_space=pltpu.HBM)
VMEM = pl.BlockSpec(memory_space=pltpu.VMEM)
SMEM = pl.BlockSpec(memory_space=pltpu.SMEM)


def params(mib):
    return pltpu.CompilerParams(vmem_limit_bytes=mib * 1024 * 1024)


def cost(flops, nbytes):
    return pl.CostEstimate(flops=int(flops), bytes_accessed=int(nbytes), transcendentals=0)


def swap_matrix(shape=(GROUP * LANES, GROUP * LANES)):
    row = lax.broadcasted_iota(jnp.int32, shape, 0)
    col = lax.broadcasted_iota(jnp.int32, shape, 1)
    swapped = (
        jnp.bitwise_and(jnp.right_shift(col, 5), 3) * LANES
        + jnp.right_shift(col, 7) * BRANCH
        + jnp.bitwise_and(col, BRANCH - 1)
    )
    return jnp.where(row == swapped, F32(1), F32(0)).astype(BF16)


def exchange(tiles):
    lane = lax.broadcasted_iota(jnp.int32, tiles[0].shape, 1)
    bit, tiles = GROUP // 2, list(tiles)
    while bit:
        width = bit * BRANCH
        low = jnp.bitwise_and(lane, width) == 0
        out = list(tiles)
        for at in range(GROUP):
            if not at & bit:
                a, b = tiles[at], tiles[at | bit]
                out[at] = jnp.where(low, a, pltpu.roll(b, width, axis=1))
                out[at | bit] = jnp.where(low, pltpu.roll(a, LANES - width, axis=1), b)
        tiles, bit = out, bit // 2
    return tiles


def pack_queries(queries_t):
    heads, width, tokens = queries_t.shape
    halves, groups, chunks = tokens // LANES, heads // GROUP, 9
    rows = width // chunks

    def body(q_hbm, out_ref, q_ref, sems, perm):
        def copy(d):
            at = pl.ds(pl.multiple_of(d * rows, 16), rows)
            return pltpu.make_async_copy(q_hbm.at[:, at, :], q_ref.at[:, at, :], sems.at[d])

        for d in range(chunks):
            copy(d).start()
        perm[...] = swap_matrix()

        @pl.loop(0, chunks)
        def _(d):
            copy(d).wait()
            at = pl.ds(pl.multiple_of(d * rows, 16), rows)
            wide = jnp.concatenate(
                [
                    jnp.concatenate(
                        [q_ref[g * GROUP + h, at, a * LANES : (a + 1) * LANES] for h in range(GROUP)],
                        axis=1,
                    )
                    for a in range(halves)
                    for g in range(groups)
                ],
                axis=0,
            )
            mixed = jnp.dot(wide, perm[...], preferred_element_type=F32).astype(BF16)
            for a in range(halves):
                for g in range(groups):
                    top = (a * groups + g) * rows
                    for b in range(GROUP):
                        out_ref[a * GROUP + b, at, g * LANES : (g + 1) * LANES] = mixed[
                            top : top + rows, b * LANES : (b + 1) * LANES
                        ]

    return pl.pallas_call(
        body,
        in_specs=[HBM],
        out_specs=VMEM,
        out_shape=jax.ShapeDtypeStruct((tokens // BRANCH, width, heads * BRANCH), BF16),
        scratch_shapes=[
            pltpu.VMEM((heads, width, tokens), BF16),
            pltpu.SemaphoreType.DMA((chunks,)),
            pltpu.VMEM((GROUP * LANES, GROUP * LANES), BF16),
        ],
        compiler_params=params(16),
        cost_estimate=cost(2 * heads * tokens * width * 512, 4 * heads * tokens * width),
        name="pack_queries",
    )(pltpu.with_memory_space_constraint(queries_t, pltpu.HBM))


def pack_grads(grad_rows, saved_rows, lse_t):
    heads, tokens = lse_t.shape
    groups = heads // GROUP
    rows, rank = grad_rows.shape
    cols = heads * BRANCH
    branches = rows // cols
    head_bits = heads.bit_length() - 1

    def body(g_hbm, o_hbm, l_hbm, out_ref, delta_ref, lse_ref, g_ref, o_ref, l_ref, sems, l_sem, perm):
        lse_copy = pltpu.make_async_copy(l_hbm, l_ref, l_sem)
        lse_copy.start()

        def copies(b):
            at = pl.ds(pl.multiple_of(b * cols, 16), cols)
            return (
                pltpu.make_async_copy(g_hbm.at[at, :], g_ref.at[at, :], sems.at[0, b]),
                pltpu.make_async_copy(o_hbm.at[at, :], o_ref.at[at, :], sems.at[1, b]),
            )

        for b in range(branches):
            for copy in copies(b):
                copy.start()
        row = lax.broadcasted_iota(jnp.int32, (cols, cols), 0)
        col = lax.broadcasted_iota(jnp.int32, (cols, cols), 1)
        source = jnp.left_shift(jnp.bitwise_and(col, BRANCH - 1), head_bits) + jnp.right_shift(col, 5)
        perm[...] = jnp.where(row == source, F32(1), F32(0)).astype(BF16)

        @pl.loop(0, branches)
        def _(b):
            for copy in copies(b):
                copy.wait()
            at = pl.ds(pl.multiple_of(b * cols, 16), cols)
            grads = g_ref[at, :]
            out_ref[b] = lax.dot_general(
                grads, perm[...], (((0,), (0,)), ((), ())), preferred_element_type=F32
            ).astype(BF16)
            delta = jnp.sum(o_ref[at, :].astype(F32) * grads.astype(F32), axis=1, keepdims=True)
            high = delta.astype(BF16)
            rest = delta - high.astype(F32)
            mid = rest.astype(BF16)
            low = (rest - mid.astype(F32)).astype(BF16)
            lane = lax.broadcasted_iota(jnp.int32, (cols, LANES), 1)
            parts = jnp.where(
                lane == 0,
                high.astype(F32),
                jnp.where(lane == 1, mid.astype(F32), jnp.where(lane == 2, low.astype(F32), F32(0))),
            ).astype(BF16)
            moved = lax.dot_general(
                parts, perm[...], (((0,), (0,)), ((), ())), preferred_element_type=F32
            )
            delta_ref[b] = moved[0:1] + moved[1:2] + moved[2:3]

        lse_copy.wait()
        for a in range(tokens // LANES):
            tile = l_ref[:, a * LANES : (a + 1) * LANES]
            picked = exchange(
                [
                    jnp.concatenate(
                        [tile[g * GROUP + h : g * GROUP + h + 1] for g in range(groups)], axis=0
                    )
                    for h in range(GROUP)
                ]
            )
            for b in range(GROUP):
                lse_ref[a * GROUP + b] = picked[b]

    return pl.pallas_call(
        body,
        in_specs=[HBM, HBM, HBM],
        out_specs=[VMEM, VMEM, VMEM],
        out_shape=[
            jax.ShapeDtypeStruct((branches, rank, cols), BF16),
            jax.ShapeDtypeStruct((branches, 1, cols), F32),
            jax.ShapeDtypeStruct((branches, groups, LANES), F32),
        ],
        scratch_shapes=[
            pltpu.VMEM((rows, rank), BF16),
            pltpu.VMEM((rows, rank), BF16),
            pltpu.VMEM((heads, tokens), F32),
            pltpu.SemaphoreType.DMA((2, branches)),
            pltpu.SemaphoreType.DMA,
            pltpu.VMEM((cols, cols), BF16),
        ],
        compiler_params=params(20),
        cost_estimate=cost(2 * rows * rank * cols, 6 * rows * rank),
        name="pack_grads",
    )(
        pltpu.with_memory_space_constraint(grad_rows, pltpu.HBM),
        pltpu.with_memory_space_constraint(saved_rows, pltpu.HBM),
        pltpu.with_memory_space_constraint(lse_t, pltpu.HBM),
    )


def attend(place, parents, own_keys, other_keys, packed_q, packed_g, lse, deltas, sizes):
    ba, ha = sizes
    columns = ba // 2
    branches, width, cols = packed_q.shape
    rank = packed_g.shape[1]
    slots, piece, _ = own_keys.shape
    prefix = 2 * slots * piece
    key_tile = min(KEY_TILE, prefix)
    tiles = prefix // key_tile
    keys_ba = prefix // ba
    width_ba = width // ba
    half = width * keys_ba // LANES
    payload = 2 * half
    part = payload // ha

    def body(place_ref, parents_ref, own_ref, other_ref, q_ref, g_ref, lse_ref, delta_ref,
             send_ref, score_ref, keys, acc_q, acc_g, pack, prob_low):
        me_ba, me_ha = place_ref[0], place_ref[1]
        me_col, me_core = jnp.right_shift(me_ba, 1), jnp.bitwise_and(me_ba, 1)

        for core_at, ref in enumerate((own_ref, other_ref)):
            for hr in range(ha):
                for zr in range(columns):
                    ba_at = 2 * jnp.bitwise_xor(me_col, zr) + jnp.bitwise_xor(me_core, core_at)
                    at = ba_at * ha + jnp.bitwise_xor(me_ha, hr)
                    keys[pl.ds(pl.multiple_of(at * piece, piece), piece), :] = ref[hr * columns + zr]
        acc_q[...] = jnp.zeros_like(acc_q)
        acc_g[...] = jnp.zeros_like(acc_g)

        @pl.loop(0, branches)
        def _(b):
            limit = parents_ref[b * BRANCH]
            lse_row = jnp.concatenate([lse_ref[b, g : g + 1] for g in range(cols // LANES)], axis=1)
            for kt in range(tiles):
                start = kt * key_tile
                for size in (key_tile // 2, key_tile):
                    low = start if size < key_tile else start + key_tile // 2
                    wanted = limit >= low
                    if size < key_tile:
                        wanted &= limit < start + key_tile // 2

                    @pl.when(wanted)
                    def _(rows=slice(start, start + size), size=size, start=start):
                        key_block = keys[rows, :]
                        for c in range(0, cols, COLUMN_CHUNK):
                            part_of = slice(c, c + COLUMN_CHUNK)
                            scores = (
                                jnp.dot(key_block, q_ref[b, :, part_of], preferred_element_type=F32)
                                * softmax_scale
                            )
                            at = start + lax.broadcasted_iota(jnp.int32, scores.shape, 0)
                            prob = jnp.where(at <= limit, jnp.exp(scores - lse_row[:, part_of]), F32(0))
                            grad_prob = jnp.dot(
                                key_block[:, :rank], g_ref[b, :, part_of], preferred_element_type=F32
                            )
                            grad_score = prob * (grad_prob - delta_ref[b, :, part_of])
                            score_ref[b, rows, part_of] = grad_score.astype(BF16)
                            prob_low[:size, part_of] = prob.astype(BF16)
                        if size < key_tile:
                            score_ref[b, start + size : start + key_tile, :] = jnp.zeros(
                                (key_tile - size, cols), BF16
                            )
                        across = (((1,), (1,)), ((), ()))
                        acc_q[:, rows] += lax.dot_general(
                            q_ref[b], score_ref[b, rows, :], across, preferred_element_type=F32
                        )
                        acc_g[:, rows] += lax.dot_general(
                            g_ref[b], prob_low[:size, :], across, preferred_element_type=F32
                        )

                @pl.when(limit < start)
                def _(start=start):
                    score_ref[b, start : start + key_tile, :] = jnp.zeros((key_tile, cols), BF16)

        acc_q[...] = acc_q[...] * softmax_scale
        acc_q[:rank, :] += acc_g[...]
        lane = lax.broadcasted_iota(jnp.int32, (half, LANES), 1)
        per_tile = LANES // keys_ba
        for at in range(ba):
            tile = acc_q[:, (at // per_tile) * LANES : (at // per_tile + 1) * LANES]
            first = at % per_tile
            block = jnp.zeros((half, LANES), F32)
            for s in range(per_tile):
                strip = tile[s * half : (s + 1) * half, :]
                shift = ((s - first) * keys_ba) % LANES
                if shift:
                    strip = pltpu.roll(strip, shift, axis=1)
                block = jnp.where((lane >= s * keys_ba) & (lane < (s + 1) * keys_ba), strip, block)
            pack[:half, :] = block
            for l in range(prefix // LANES):
                pack[half + l * width_ba : half + (l + 1) * width_ba, :] = acc_q[
                    at * width_ba : (at + 1) * width_ba, l * LANES : (l + 1) * LANES
                ]
            to_core = jnp.bitwise_xor(me_core, at % 2)
            to_col = jnp.bitwise_xor(me_col, at // 2)
            for h in range(ha):
                send_ref[to_core, jnp.bitwise_xor(me_ha, h), to_col] = pack[
                    h * part : (h + 1) * part, :
                ]

    return pl.pallas_call(
        body,
        in_specs=[SMEM, SMEM] + [VMEM] * 6,
        out_specs=[VMEM, VMEM, VMEM],
        out_shape=[
            jax.ShapeDtypeStruct((2, ha, columns, part, LANES), F32),
            jax.ShapeDtypeStruct((branches, prefix, cols), BF16),
            jax.ShapeDtypeStruct((prefix, width), BF16),
        ],
        scratch_shapes=[
            pltpu.VMEM((width, prefix), F32),
            pltpu.VMEM((rank, prefix), F32),
            pltpu.VMEM((payload, LANES), F32),
            pltpu.VMEM((key_tile, cols), BF16),
        ],
        compiler_params=params(24),
        cost_estimate=cost(8 * branches * cols * prefix * width, 3 * branches * cols * width * 2),
        name="attend",
    )(place, parents, own_keys, other_keys, packed_q, packed_g, lse, deltas)


def query_gradient(before, steps, keys, grad_score, heads):
    branches, prefix, _ = grad_score.shape
    width = keys.shape[1]
    tokens = branches * BRANCH
    halves = tokens // LANES
    first, last = steps

    def body(k_ref, s_ref, *refs):
        out_hbm, keys_t, slots, sems = refs[-4:]
        keys_t[...] = jnp.transpose(k_ref[...], (1, 0))

        def copy(g):
            at = (g - first) % 2
            return pltpu.make_async_copy(
                slots.at[at], out_hbm.at[pl.ds(g * GROUP, GROUP)], sems.at[at]
            )

        for g in range(first, last):
            if g - first >= 2:
                copy(g - 2).wait()
            for a in range(halves):
                wide = jnp.concatenate(
                    [s_ref[a * GROUP + b, :, g * LANES : (g + 1) * LANES] for b in range(GROUP)], axis=1
                )
                grads = softmax_scale * jnp.dot(keys_t[...], wide, preferred_element_type=F32)
                tiles = exchange([grads[:, b * LANES : (b + 1) * LANES] for b in range(GROUP)])
                for h in range(GROUP):
                    slots[(g - first) % 2, h, :, a * LANES : (a + 1) * LANES] = tiles[h].astype(BF16)
            copy(g).start()
        for g in range(max(first, last - 2), last):
            copy(g).wait()

    return pl.pallas_call(
        body,
        in_specs=[VMEM, VMEM] + ([] if before is None else [HBM]),
        out_specs=HBM,
        out_shape=jax.ShapeDtypeStruct((heads, width, tokens), BF16),
        input_output_aliases={} if before is None else {2: 0},
        scratch_shapes=[
            pltpu.VMEM((width, prefix), BF16),
            pltpu.VMEM((2, GROUP, width, tokens), BF16),
            pltpu.SemaphoreType.DMA((2,)),
        ],
        compiler_params=params(16),
        cost_estimate=cost(
            2 * (last - first) * GROUP * tokens * prefix * width, (last - first) * GROUP * tokens * width * 2
        ),
        name="query_gradient",
    )(keys, grad_score, *([] if before is None else [before]))


def project(place, parts, hidden_sets, order, latent_weight, sizes, prefix):
    ba, ha = sizes
    width, columns = latent_weight.shape
    keys_ba, width_ba = prefix // ba, width // ba
    part = parts[0].shape[0]
    half = part * ha // 2
    middle = -(-columns // 512) * 256
    parts_of = (slice(0, middle), slice(middle, columns))

    def body(place_ref, *refs):
        part_refs = refs[:ha]
        own_ref, other_ref, weight_ref, wgrad_hbm, igrad_hbm, pack, hid, wrows, irows, sems = refs[ha:]
        me_ba, me_ha = place_ref[0], place_ref[1]
        for hr in range(ha):
            at = jnp.bitwise_xor(me_ha, hr) * part
            pack[pl.ds(pl.multiple_of(at, 8), part), :] = part_refs[hr][...].astype(F32)
        for core_at, ref in enumerate((own_ref, other_ref)):
            for slot, zr in enumerate(order):
                at = jnp.bitwise_xor(me_ba, 2 * zr + core_at) * keys_ba
                hid[pl.ds(pl.multiple_of(at, 8), keys_ba), :] = ref[slot]
        grad_columns = jnp.concatenate(
            [
                pack[half + l * width_ba : half + (l + 1) * width_ba, :]
                for l in range(prefix // LANES)
            ],
            axis=1,
        ).astype(BF16)
        rows_t = jnp.concatenate(
            [
                pack[:half, s * keys_ba : (s + 1) * keys_ba]
                for s in range(LANES // keys_ba)
            ],
            axis=0,
        ).astype(BF16)
        copies = []

        def send(buffer, out_hbm, at, value):
            buffer[:, at] = value.astype(BF16)
            copy = pltpu.make_async_copy(buffer.at[:, at], out_hbm.at[:, at], sems.at[len(copies)])
            copy.start()
            copies.append(copy)

        for at in parts_of:
            term = lax.dot_general(
                rows_t, weight_ref[:, at], (((0,), (0,)), ((), ())), preferred_element_type=F32
            )
            send(irows, igrad_hbm, at, term)
        for at in parts_of:
            send(wrows, wgrad_hbm, at, jnp.dot(grad_columns, hid[:, at], preferred_element_type=F32))
        for copy in copies:
            copy.wait()

    return pl.pallas_call(
        body,
        in_specs=[SMEM] + [VMEM] * (ha + 3),
        out_specs=[HBM, HBM],
        out_shape=[
            jax.ShapeDtypeStruct((width_ba, columns), BF16),
            jax.ShapeDtypeStruct((keys_ba, columns), BF16),
        ],
        scratch_shapes=[
            pltpu.VMEM((part * ha, LANES), F32),
            pltpu.VMEM((prefix, columns), BF16),
            pltpu.VMEM((width_ba, columns), BF16),
            pltpu.VMEM((keys_ba, columns), BF16),
            pltpu.SemaphoreType.DMA((4,)),
        ],
        compiler_params=params(24),
        cost_estimate=cost(4 * width * keys_ba * columns, 4 * width * columns),
        name="project",
    )(place, *parts, *hidden_sets, latent_weight)


def on_device(sizes, queries, out_grad, out_saved, logsumexp, parents, latents, hidden, latent_weight):
    ba, ha = sizes
    columns = ba // 2
    tokens, heads, _ = queries.shape
    rank = out_grad.shape[2]
    prefix = latents.shape[0] * ba * ha

    def over_core(x):
        return lax.ppermute(x, "ba", [(i, i ^ 1) for i in range(ba)])

    def over_column(x, k):
        return lax.ppermute(x, "ba", [(i, i ^ (2 * k)) for i in range(ba)])

    def over_ha(x, k):
        return lax.ppermute(x, "ha", [(i, i ^ k) for i in range(ha)])

    def total(terms):
        return sum(t.astype(F32) for t in terms).astype(BF16)

    place = jnp.stack([lax.axis_index("ba"), lax.axis_index("ha")]).astype(jnp.int32)

    keys = jnp.stack([latents] + [over_column(latents, k) for k in range(1, columns)])
    keys = lax.optimization_barrier(keys)
    keys = jnp.concatenate([keys] + [over_ha(keys, k) for k in range(1, ha)])
    other_keys = over_core(keys)

    packed_q = pack_queries(jnp.transpose(queries, (1, 2, 0)))
    packed_g, deltas, lse = pack_grads(
        out_grad.reshape(tokens * heads, rank), out_saved.reshape(tokens * heads, rank), logsumexp.T
    )

    hidden_all, order = hidden[None], [0]
    step = columns // 2
    while step:
        hidden_all = jnp.concatenate([hidden_all, over_column(hidden_all, step)])
        if step > 1:
            place, hidden_all = lax.optimization_barrier((place, hidden_all))
        order = order + [k ^ step for k in order]
        step //= 2
    other_hidden = over_core(hidden_all)

    send, grad_score, keys = attend(
        place, parents, keys, other_keys, packed_q, packed_g, lse, deltas, sizes
    )
    query_grad, groups = None, heads // GROUP
    for steps in ((0, 1), (1, groups)):
        query_grad = query_gradient(query_grad, steps, keys, grad_score, heads)

    chip = (send[0] + over_core(send[1])).astype(BF16)
    plane = total([chip[0]] + [over_ha(chip[k], k) for k in range(1, ha)])
    owned = total([plane[0]] + [over_column(plane[k], k) for k in range(1, columns)])
    parts = [owned] + [over_ha(owned, k) for k in range(1, ha)]
    weight_grad, input_grad = project(
        place, parts, (hidden_all, other_hidden), order, latent_weight, sizes, prefix
    )
    return (jnp.transpose(query_grad, (2, 0, 1)), weight_grad, input_grad)


def solution(mesh):
    sizes = (mesh.shape["ba"], mesh.shape["ha"])

    def step(*args):
        return on_device(sizes, *args)

    step = jax.shard_map(
        step,
        mesh=mesh,
        in_specs=(
            P("ba", "ha", None),
            P("ba", "ha", None),
            P("ba", "ha", None),
            P("ba", "ha"),
            P("ba"),
            P(("ba", "ha"), None),
            P("ba", "ha"),
            P(None, "ha"),
        ),
        out_specs=(P("ba", "ha", None), P("ba", "ha"), P("ba", "ha")),
        check_vma=False,
    )
    return step
```
